512 devices in a mesh: child: 16 (over x, z_lo), shard: 32 (over y, z_hi, core).
Axes of the slice: x: 4, y: 4, z: 16 (z_hi: 4, z_lo: 4; z = z_hi * 4 + z_lo), core: 2. Of those that a mesh axis runs over, the one named last changes fastest.
Arguments:
- child_tensors: bfloat16 [16, 256, 256, 256], P('child', 'shard'), may hold values from -6 to 6
- leg_ops: bfloat16 [8, 256, 256], replicated, may hold values from -0.375 to 0.375
- term_ops: int32 [16, 4, 2], P('child'), may hold values from 0 to 7
- term_coef: float32 [16, 4], P('child'), may hold values from 0.5 to 1.5
- parent: bfloat16 [16, 256, 256], P('child', 'shard'), may hold values from -0.375 to 0.375
- top_env: float32 [256, 256], replicated, may hold values from -6 to 6
Outputs:
- applied: bfloat16 [16, 256, 256, 256], P('child', None, 'shard')
The draws below stay inside these ranges and needn't reach their ends.
Inputs may be any that keep to these rules, and one draw needn't show every extreme that they name: `term_ops`: each entry names one of the 8 leg operators.
All inputs are finite; a program needn't handle non-finite values.
Results may differ from the reference program's by a relative error of at most 0.0091.
Values may be sent and summed in bfloat16 or wider, within the bound.
No kernel may reach another device: no remote copies, remote signals or barrier semaphores. Data moves between devices by JAX's collectives and lax.ppermute only.
A program may use at most 64 MiB of HBM per device.

```python
import math
import jax
import jax.numpy as jnp
from jax import lax

B = 256
TPC = 4
NOPS = 8
CHILDREN = 16


def place_ends(array, own_key, least, high):
    place = [jax.random.randint(jax.random.fold_in(own_key, axis), (), 0, length) for axis, length in enumerate(array.shape)]
    widest = array.shape.index(max(array.shape))
    beside = place[:widest] + [(place[widest] + 1) % array.shape[widest]] + place[widest + 1:]
    return array.at[tuple(place)].set(least).at[tuple(beside)].set(high)


def level_of(key, extent, split, least, largest):
    gain = 1.0
    for axis_at, parts in split:
        steps = jax.random.uniform(jax.random.fold_in(jax.random.fold_in(key, 6), axis_at), (parts,), jnp.float32, least / len(split), largest / len(split))
        gain = gain * jnp.repeat(jnp.exp(steps), extent[axis_at] // parts).reshape((-1,) + (1,) * (len(extent) - 1 - axis_at))
    return gain


def gaussian(key, dims, spread, most, cuts=(), kind=jnp.bfloat16):
    result = spread * jax.random.normal(key, dims, jnp.float32)
    if cuts:
        result = result * level_of(key, dims, cuts, -0.22, 0.18)
    return jnp.clip(result, -most, most).astype(kind)


def setup_inputs(seed: int = 0) -> dict:
    streams_of = jax.random.split(jax.random.key(seed), 7)
    child_tensors = gaussian(streams_of[0], (CHILDREN, B, B, B), 1.0, 6.0, ((0, 16), (1, 32)))
    leg_ops = gaussian(streams_of[1], (NOPS, B, B), B ** -0.5, 0.375)
    term_ops = place_ends(jax.random.randint(streams_of[2], (CHILDREN, TPC, 2), 0, NOPS), jax.random.fold_in(streams_of[2], 1), 0, NOPS - 1).astype(jnp.int32)
    term_coef = jnp.clip(0.5 + 1.0 * jax.random.uniform(streams_of[3], (CHILDREN, TPC), jnp.float32) ** level_of(streams_of[3], (CHILDREN, TPC), ((0, 16),), -0.2, 0.2), 0.5, 1.5)
    parent = gaussian(streams_of[4], (CHILDREN, B, B), B ** -0.5, 0.375, ((0, 16), (1, 32)))
    top_env = gaussian(streams_of[5], (B, B), 1.0, 6.0, (), jnp.float32)
    return dict(child_tensors=child_tensors, leg_ops=leg_ops, term_ops=term_ops, term_coef=term_coef, parent=parent, top_env=top_env)


def reference(child_tensors, leg_ops, term_ops, term_coef, parent, top_env):
    high = lax.Precision.HIGHEST
    bank = leg_ops.astype(jnp.float32)

    def first(item):
        tensor, picks, weights, block = item
        dense = tensor.astype(jnp.float32)
        lift = block.astype(jnp.float32)
        local = jnp.zeros((B, B, B), jnp.float32)
        for term in range(TPC):
            right = bank[picks[term, 1]]
            left = bank[picks[term, 0]]
            image = jnp.einsum('lru,rs->lsu', dense, right, precision=high).astype(jnp.bfloat16)
            image = lax.optimization_barrier(image).astype(jnp.float32)
            local = local + weights[term] * jnp.einsum('lk,lsu->ksu', left, image, precision=high)
        rounded = lax.optimization_barrier(local.astype(jnp.bfloat16)).astype(jnp.float32)
        env = jnp.einsum('lsu,lsv->uv', dense, rounded, precision=high) / B
        lifted = jnp.dot(lift.T, jnp.dot(env, lift, precision=high), precision=high)
        return (local, lifted)
    locals_all, lifted_all = lax.map(first, (child_tensors, term_ops, term_coef, parent))
    total = lax.optimization_barrier(jnp.sum(lifted_all, axis=0))
    factor = 1.0 / math.sqrt(B * CHILDREN)

    def second(item):
        tensor, local, block, own = item
        lift = block.astype(jnp.float32)
        coupling = total - own + top_env
        hole = jnp.dot(jnp.dot(lift, coupling, precision=high), lift.T, precision=high) * factor
        hole = hole.astype(jnp.bfloat16).astype(jnp.float32)
        moved = jnp.einsum('lsu,uv->lsv', tensor.astype(jnp.float32), hole, precision=high)
        return (local + moved).astype(jnp.bfloat16)
    return lax.map(second, (child_tensors, locals_all, parent, lifted_all))
```

```python
import math

import jax
import jax.numpy as jnp
from jax import lax
from jax.experimental import pallas as pl
from jax.experimental.pallas import tpu as pltpu
from jax.sharding import Mesh, PartitionSpec as P


X, ZL, Y, ZH, C = 4, 4, 4, 4, 2
PLANE = ("x", "y", "c")
LINE = ("zl", "zh")
HIGH = lax.Precision.HIGHEST
F32 = jnp.float32
BF16 = jnp.bfloat16


def exchange(parts, axes):
    return lax.all_to_all(parts, axes, 0, 0, tiled=True)


def shifted(piece, shift):
    return lax.ppermute(piece, "zh", [(i, (i + shift) % ZH) for i in range(ZH)])


def tied(*values):
    return lax.optimization_barrier(values)


def local_kernel(picks, coefs, tensor, bank, bank_t, out):
    def column(u, carry):
        block = tensor[u]
        total = None
        for term in range(picks.shape[0]):
            right = bank[picks[term, 1]]
            left = bank_t[picks[term, 0]]
            image = jnp.dot(block, right, preferred_element_type=F32).astype(BF16)
            part = coefs[term] * jnp.dot(left, image, preferred_element_type=F32)
            total = part if total is None else total + part
        out[u] = total.astype(out.dtype)
        return carry

    lax.fori_loop(0, tensor.shape[0], column, 0)


def local_columns(tensor, bank, bank_t, picks, coefs):
    blk, bond, _ = tensor.shape
    flops = 4 * blk * bond**3 * picks.shape[0]
    return pl.pallas_call(
        local_kernel,
        out_shape=jax.ShapeDtypeStruct((blk, bond, bond), BF16),
        in_specs=[pl.BlockSpec(memory_space=pltpu.SMEM)] * 2
        + [pl.BlockSpec(memory_space=pltpu.VMEM)] * 3,
        out_specs=pl.BlockSpec(memory_space=pltpu.VMEM),
        cost_estimate=pl.CostEstimate(
            flops=flops, bytes_accessed=8 * blk * bond * bond, transcendentals=0
        ),
        name="local_columns",
    )(picks, coefs, tensor, bank, bank_t)


def result_kernel(right, hole, arrived, out):
    lines = 256

    def chunk(i, carry):
        at = pl.ds(pl.multiple_of(i * lines, lines), lines)
        moved = jnp.dot(right[at, :], hole[...], preferred_element_type=F32)
        out[at, :] = (arrived[at, :].astype(F32) + moved).astype(out.dtype)
        return carry

    lax.fori_loop(0, right.shape[0] // lines, chunk, 0)


def result_rows(right, hole, arrived):
    rows, bond = right.shape
    return pl.pallas_call(
        result_kernel,
        out_shape=jax.ShapeDtypeStruct((rows, bond), BF16),
        in_specs=[pl.BlockSpec(memory_space=pltpu.VMEM)] * 3,
        out_specs=pl.BlockSpec(memory_space=pltpu.VMEM),
        cost_estimate=pl.CostEstimate(
            flops=2 * rows * bond * bond, bytes_accessed=6 * rows * bond, transcendentals=0
        ),
        name="result_rows",
    )(right, hole, arrived)


def body(child_tensors, leg_ops, term_ops, term_coef, parent, top_env):
    x, zl, zh = lax.axis_index("x"), lax.axis_index("zl"), lax.axis_index("zh")
    plane = (x * Y + lax.axis_index("y")) * C + lax.axis_index("c")
    tensor = child_tensors[0]
    blk, bond, _ = tensor.shape
    rows = parent[0]
    terms = term_coef.shape[1]

    turned = tensor.transpose(2, 0, 1).reshape(X * Y * C, blk, blk, bond)
    own_rows = jnp.broadcast_to(rows[None, None], (X * Y * C, 1, blk, bond))
    met = exchange(jnp.concatenate([turned, own_rows], axis=1), PLANE)

    by_leg = tensor.reshape(blk, Y, ZH, C, blk, bond)

    def for_right(shift):
        piece = lax.dynamic_index_in_dim(by_leg, (zh + shift) % ZH, 2, keepdims=False)
        return piece.transpose(1, 2, 0, 3, 4).reshape(Y * C, blk, blk, bond)

    near_1, near_3 = shifted(for_right(1), 1), shifted(for_right(3), 3)
    met, near_1, near_3 = tied(met, near_1, near_3)
    met = met.reshape(X, Y * C, blk + 1, blk, bond)

    def for_plane(shift):
        return lax.dynamic_index_in_dim(met, (zh + shift) % ZH, 0, keepdims=False)

    home = jnp.zeros((Y, ZH, C, blk + 1, blk, bond), BF16)
    moved = [for_plane(0)] + [shifted(for_plane(s), s) for s in (1, 3, 2)]
    for s, piece in zip((0, 1, 3, 2), moved):
        piece = piece.reshape(Y, 1, C, blk + 1, blk, bond)
        home = lax.dynamic_update_slice_in_dim(home, piece, (zh - s) % ZH, 1)
    home = home.reshape(Y * ZH * C, blk + 1, blk, bond)
    home_t = home[:, :blk]
    home_p = home[:, blk].reshape(bond, bond).astype(F32)

    said = jnp.concatenate([term_ops[0].astype(F32), term_coef[0][:, None]], axis=1)
    said = jnp.pad(said, ((0, 8 - terms), (0, 125)))
    said, _ = tied(said, met)
    heard = exchange(jnp.broadcast_to(said[None], (X, 8, 128)), ("x",))
    mine = lax.dynamic_index_in_dim(heard, zh, 0, keepdims=False)
    picks = mine[:terms, :2].astype(jnp.int32)
    coefs = mine[:terms, 2]

    near, _ = tied(jnp.stack([for_right(0), near_1, near_3], axis=1), met)
    near = exchange(near, ("y", "c"))
    far, _ = tied(for_right(2), near)
    far = exchange(far, ("y", "c"))

    own_p = lax.dynamic_index_in_dim(met[:, :, blk], x, 0, keepdims=False)
    own_p, _ = tied(own_p, near)
    block_p = jnp.zeros((Y, ZH, C, blk, bond), BF16)
    for s in (0, 1, 3, 2):
        piece = (shifted(own_p, s) if s else own_p).reshape(Y, 1, C, blk, bond)
        block_p = lax.dynamic_update_slice_in_dim(block_p, piece, (zh - s) % ZH, 1)
    block_p = block_p.reshape(bond, bond).astype(F32)

    columns = home_t.transpose(1, 0, 2, 3).reshape(blk, bond, bond)
    columns, near, far = tied(columns, near, far)
    far = shifted(far, 2)
    local = local_columns(columns, leg_ops, leg_ops.transpose(0, 2, 1), picks, coefs)

    leaving = local.reshape(blk, bond, Y, ZH, C, blk).transpose(3, 2, 4, 0, 5, 1)

    def for_away(shift):
        return lax.dynamic_index_in_dim(leaving, (zh + shift) % ZH, 0, keepdims=False)

    away = jnp.zeros((X, Y, C, blk, blk, bond), BF16)
    for s in (0, 1, 3, 2):
        piece = shifted(for_away(s), s) if s else for_away(s)
        away = lax.dynamic_update_slice_in_dim(away, piece[None], (zh - s) % ZH, 0)

    local_rows = local.reshape(blk, bond // blk, blk, bond).transpose(1, 0, 2, 3)
    both = exchange(jnp.concatenate([home_t, local_rows], axis=1), PLANE)
    bra = both[:, :blk].reshape(bond, blk, bond)
    ket = both[:, blk:].reshape(bond, blk, bond)
    env = jnp.einsum("ulr,vlr->uv", bra, ket, preferred_element_type=F32) / bond
    lifted = jnp.dot(home_p.T, jnp.dot(env, home_p, precision=HIGH), precision=HIGH)
    lifted = exchange(lifted.astype(BF16).reshape(X * Y * C, blk, bond), PLANE)
    lifted = lifted.astype(F32).sum(axis=0)
    everyone = exchange(jnp.broadcast_to(lifted[None], (ZL * ZH, blk, bond)), LINE)
    total = everyone.sum(axis=0)
    mates = lax.dynamic_index_in_dim(
        everyone.reshape(ZL, ZH, blk, bond), zl, 0, keepdims=False
    )
    top_rows = lax.dynamic_slice_in_dim(top_env, plane * blk, blk, 0)
    coupling = ((total + top_rows)[None] - mates).astype(BF16)
    coupling = jnp.broadcast_to(coupling[:, None], (X, Y * C, blk, bond))
    coupling = exchange(coupling.reshape(X * Y * C, blk, bond), PLANE)
    coupling = coupling.reshape(bond, bond).astype(F32)
    factor = 1.0 / math.sqrt(bond * X * ZL)
    hole = jnp.dot(jnp.dot(block_p, coupling, precision=HIGH), block_p.T, precision=HIGH)
    hole = (hole * factor).astype(BF16)

    right = jnp.zeros((Y, ZH, C, blk, blk, bond), BF16)
    for s, piece in ((0, near[:, 0]), (1, near[:, 1]), (3, near[:, 2]), (2, far)):
        piece = piece.reshape(Y, 1, C, blk, blk, bond)
        right = lax.dynamic_update_slice_in_dim(right, piece, (zh - s) % ZH, 1)
    right = right.reshape(bond * blk, bond)
    away, _ = tied(away.reshape(X * Y * C, blk, blk, bond), coupling)
    arrived = exchange(away, PLANE).reshape(bond, blk, bond)
    arrived = arrived.transpose(2, 1, 0).reshape(bond * blk, bond)
    return result_rows(right, hole, arrived).reshape(1, bond, blk, bond)


def solution(mesh):
    fine = Mesh(mesh.devices.reshape(X, ZL, Y, ZH, C), ("x", "zl", "y", "zh", "c"))
    child, shard = ("x", "zl"), ("y", "zh", "c")
    in_specs = (
        P(child, shard, None, None),
        P(),
        P(child, None, None),
        P(child, None),
        P(child, shard, None),
        P(),
    )
    out_specs = P(child, None, shard, None)
    return jax.shard_map(
        body, mesh=fine, in_specs=in_specs, out_specs=out_specs, check_vma=False
    )
```

```python
import math

import jax
import jax.numpy as jnp
from jax import lax
from jax.experimental import pallas as pl
from jax.experimental.pallas import tpu as pltpu
from jax.sharding import Mesh, PartitionSpec as P

X, ZL, Y, ZH, C = 4, 4, 4, 4, 2
SHARD = ("y", "zh", "c")
PLANE = ("x", "y", "c")
LINE = ("zl", "zh")
HIGH = lax.Precision.HIGHEST
F32 = jnp.float32
BF16 = jnp.bfloat16


def exchange(parts, axes):
    return lax.all_to_all(parts, axes, 0, 0, tiled=True)


def local_kernel(picks, coefs, tensor, bank, bank_t, out):
    def column(u, carry):
        block = tensor[u]
        total = None
        for term in range(picks.shape[0]):
            left = bank[picks[term, 0]]
            right = bank_t[picks[term, 1]]
            image = jax.lax.dot_general(
                right, block, (((1,), (1,)), ((), ())), preferred_element_type=F32
            ).astype(BF16)
            part = coefs[term] * jnp.dot(image, left, preferred_element_type=F32)
            total = part if total is None else total + part
        out[u] = total.astype(out.dtype)
        return carry

    lax.fori_loop(0, tensor.shape[0], column, 0)


def local_columns(tensor, bank, bank_t, picks, coefs):
    blk, bond, _ = tensor.shape
    flops = 4 * blk * bond**3 * picks.shape[0]
    return pl.pallas_call(
        local_kernel,
        out_shape=jax.ShapeDtypeStruct((blk, bond, bond), BF16),
        in_specs=[pl.BlockSpec(memory_space=pltpu.SMEM)] * 2
        + [pl.BlockSpec(memory_space=pltpu.VMEM)] * 3,
        out_specs=pl.BlockSpec(memory_space=pltpu.VMEM),
        cost_estimate=pl.CostEstimate(
            flops=flops, bytes_accessed=8 * blk * bond * bond, transcendentals=0
        ),
        compiler_params=pltpu.CompilerParams(vmem_limit_bytes=16 * 2**20),
        name="local_columns",
    )(picks, coefs, tensor, bank, bank_t)


def result_kernel(right, hole, arrived, out):
    lines = 256

    def chunk(i, carry):
        at = pl.ds(pl.multiple_of(i * lines, lines), lines)
        moved = jnp.dot(right[at, :], hole[...], preferred_element_type=F32)
        out[at, :] = (arrived[at, :].astype(F32) + moved).astype(out.dtype)
        return carry

    lax.fori_loop(0, right.shape[0] // lines, chunk, 0)


def result_rows(right, hole, arrived):
    rows, bond = right.shape
    return pl.pallas_call(
        result_kernel,
        out_shape=jax.ShapeDtypeStruct((rows, bond), BF16),
        in_specs=[pl.BlockSpec(memory_space=pltpu.VMEM)] * 3,
        out_specs=pl.BlockSpec(memory_space=pltpu.VMEM),
        cost_estimate=pl.CostEstimate(
            flops=2 * rows * bond * bond, bytes_accessed=6 * rows * bond, transcendentals=0
        ),
        compiler_params=pltpu.CompilerParams(vmem_limit_bytes=16 * 2**20),
        name="result_rows",
    )(right, hole, arrived)


def shards(child_tensors, leg_ops, term_ops, term_coef, parent, top_env):
    zl = lax.axis_index("zl")
    plane = (lax.axis_index("x") * Y + lax.axis_index("y")) * C + lax.axis_index("c")
    tensor = child_tensors[0]
    blk, bond, _ = tensor.shape
    devices = Y * ZH * C

    turned = tensor.transpose(2, 0, 1).reshape(devices, blk, blk, bond)
    columns = exchange(turned, SHARD).transpose(1, 0, 2, 3).reshape(blk, bond, bond)

    rows = jnp.broadcast_to(parent[0][None, None], (devices, 1, blk, bond))
    blocks = tensor.reshape(blk, devices, blk, bond).transpose(1, 0, 2, 3)
    blocks = exchange(jnp.concatenate([blocks, rows], axis=1), SHARD)
    right = blocks[:, :blk].reshape(bond * blk, bond)
    lift = blocks[:, blk].reshape(bond, bond).astype(F32)

    local = local_columns(columns, leg_ops, leg_ops.transpose(0, 2, 1), term_ops[0], term_coef[0])
    local = local.reshape(blk, devices, blk, bond).transpose(1, 0, 2, 3)
    local = exchange(local, SHARD).reshape(bond, blk, bond)
    local = local.transpose(2, 1, 0).reshape(bond * blk, bond)

    env = jnp.einsum("pu,pv->uv", right, local, preferred_element_type=F32) / bond
    lifted = jnp.dot(lift.T, jnp.dot(env, lift, precision=HIGH), precision=HIGH)

    lifted = exchange(lifted.astype(BF16).reshape(X * Y * C, blk, bond), PLANE)
    lifted = lifted.reshape(X, Y * C, blk, bond).astype(F32).sum(axis=1).astype(BF16)
    lifted = exchange(jnp.broadcast_to(lifted[None], (ZL * ZH, X, blk, bond)), LINE)
    lifted = lifted.reshape(ZL, ZH, X, blk, bond).astype(F32).sum(axis=1)
    total = lifted.sum(axis=(0, 1))
    mates = lax.dynamic_index_in_dim(lifted, zl, 0, keepdims=False)
    top_rows = lax.dynamic_slice_in_dim(top_env, plane * blk, blk, 0)
    coupling = ((total + top_rows)[None] - mates).astype(BF16)
    coupling = jnp.broadcast_to(coupling[:, None], (X, Y * C, blk, bond))
    coupling = exchange(coupling.reshape(X * Y * C, blk, bond), PLANE)
    coupling = coupling.reshape(bond, bond).astype(F32)
    factor = 1.0 / math.sqrt(bond * X * ZL)
    hole = jnp.dot(jnp.dot(lift, coupling, precision=HIGH), lift.T, precision=HIGH)
    hole = (hole * factor).astype(BF16)

    return result_rows(right, hole, local).reshape(1, bond, blk, bond)


def solution(mesh):
    fine = Mesh(mesh.devices.reshape(X, ZL, Y, ZH, C), ("x", "zl", "y", "zh", "c"))
    child, shard = ("x", "zl"), ("y", "zh", "c")
    in_specs = (
        P(child, shard, None, None),
        P(),
        P(child, None, None),
        P(child, None),
        P(child, shard, None),
        P(),
    )
    out_specs = P(child, None, shard, None)
    return jax.shard_map(shards, mesh=fine, in_specs=in_specs, out_specs=out_specs, check_vma=False)
```

```python
import math

import jax
import jax.numpy as jnp
from jax import lax
from jax.experimental import pallas as pl
from jax.experimental.pallas import tpu as pltpu
from jax.sharding import Mesh, PartitionSpec as P


X, ZL, Y, ZH, C = 4, 4, 4, 4, 2
SHARD = ("y", "zh", "c")
PLANE = ("x", "y", "c")
LINE = ("zl", "zh")
HIGH = lax.Precision.HIGHEST
F32 = jnp.float32
BF16 = jnp.bfloat16


def exchange(parts, axes):
    return lax.all_to_all(parts, axes, 0, 0, tiled=True)


def shifted(piece, shift):
    return lax.ppermute(piece, "zh", [(i, (i + shift) % ZH) for i in range(ZH)])


def tied(*values):
    return lax.optimization_barrier(values)


def local_kernel(picks, coefs, tensor, bank, bank_t, out):
    def column(u, carry):
        block = tensor[u]
        total = None
        for term in range(picks.shape[0]):
            right = bank[picks[term, 1]]
            left = bank_t[picks[term, 0]]
            image = jnp.dot(block, right, preferred_element_type=F32).astype(BF16)
            part = coefs[term] * jnp.dot(left, image, preferred_element_type=F32)
            total = part if total is None else total + part
        out[u] = total.astype(out.dtype)
        return carry

    lax.fori_loop(0, tensor.shape[0], column, 0)


def local_columns(tensor, bank, bank_t, picks, coefs):
    blk, bond, _ = tensor.shape
    flops = 4 * blk * bond**3 * picks.shape[0]
    return pl.pallas_call(
        local_kernel,
        out_shape=jax.ShapeDtypeStruct((blk, bond, bond), BF16),
        in_specs=[pl.BlockSpec(memory_space=pltpu.SMEM)] * 2
        + [pl.BlockSpec(memory_space=pltpu.VMEM)] * 3,
        out_specs=pl.BlockSpec(memory_space=pltpu.VMEM),
        cost_estimate=pl.CostEstimate(
            flops=flops, bytes_accessed=8 * blk * bond * bond, transcendentals=0
        ),
        compiler_params=pltpu.CompilerParams(vmem_limit_bytes=16 * 2**20),
        name="local_columns",
    )(picks, coefs, tensor, bank, bank_t)


def result_kernel(right, hole, arrived, out):
    lines = 256

    def chunk(i, carry):
        at = pl.ds(pl.multiple_of(i * lines, lines), lines)
        moved = jnp.dot(right[at, :], hole[...], preferred_element_type=F32)
        out[at, :] = (arrived[at, :].astype(F32) + moved).astype(out.dtype)
        return carry

    lax.fori_loop(0, right.shape[0] // lines, chunk, 0)


def result_rows(right, hole, arrived):
    rows, bond = right.shape
    return pl.pallas_call(
        result_kernel,
        out_shape=jax.ShapeDtypeStruct((rows, bond), BF16),
        in_specs=[pl.BlockSpec(memory_space=pltpu.VMEM)] * 3,
        out_specs=pl.BlockSpec(memory_space=pltpu.VMEM),
        cost_estimate=pl.CostEstimate(
            flops=2 * rows * bond * bond, bytes_accessed=6 * rows * bond, transcendentals=0
        ),
        compiler_params=pltpu.CompilerParams(vmem_limit_bytes=16 * 2**20),
        name="result_rows",
    )(right, hole, arrived)


def body(child_tensors, leg_ops, term_ops, term_coef, parent, top_env):
    x, zl, zh = lax.axis_index("x"), lax.axis_index("zl"), lax.axis_index("zh")
    plane = (x * Y + lax.axis_index("y")) * C + lax.axis_index("c")
    tensor = child_tensors[0]
    blk, bond, _ = tensor.shape
    rows = parent[0]
    terms = term_coef.shape[1]
    mates_n = Y * C

    high = lax.reduce_precision(term_coef[0], 8, 7)
    mid = lax.reduce_precision(term_coef[0] - high, 8, 7)
    low = term_coef[0] - high - mid
    told = jnp.concatenate([term_ops[0].reshape(-1).astype(F32), high, mid, low]).astype(BF16)
    told = jnp.pad(told[None], ((0, blk - 1), (0, bond - 5 * terms)))
    turned = tensor.transpose(2, 0, 1).reshape(X, bond // X, blk, bond)
    extra = jnp.broadcast_to(jnp.stack([rows, told])[None], (X, 2, blk, bond))
    met = exchange(jnp.concatenate([turned, extra], axis=1), ("x",))
    met_rows = met[:, bond // X]
    heard = lax.dynamic_index_in_dim(met[:, bond // X + 1], zh, 0, keepdims=False)[0].astype(F32)
    picks = heard[: 2 * terms].reshape(terms, 2).astype(jnp.int32)
    coefs = heard[2 * terms : 5 * terms].reshape(3, terms).sum(axis=0)

    met = met[:, : bond // X].reshape(X, Y, C, blk, blk, bond).transpose(1, 0, 2, 3, 4, 5)
    home = exchange(met.reshape(Y * ZH * C, blk, blk, bond), SHARD)

    by_leg = tensor.reshape(blk, Y, ZH, C, blk, bond)

    def for_right(shift):
        piece = lax.dynamic_index_in_dim(by_leg, (zh + shift) % ZH, 2, keepdims=False)
        piece = piece.transpose(1, 2, 0, 3, 4).reshape(mates_n * blk, blk, bond)
        return jnp.concatenate([piece, rows[None]], axis=0)

    def for_home(shift):
        return lax.dynamic_index_in_dim(met_rows, (zh + shift) % X, 0)

    legs = {s: for_right(s) for s in range(ZH)}
    parts = {s: for_home(s) for s in range(ZH)}
    for s in (1, 3, 2):
        parts[s] = shifted(parts[s], s)
    for s in (1, 3):
        legs[s] = shifted(legs[s], s)
    home_rows = jnp.zeros((ZH, blk, bond), BF16)
    for s in range(ZH):
        home_rows = lax.dynamic_update_slice_in_dim(home_rows, parts[s], (zh - s) % ZH, 0)

    columns = home.transpose(1, 0, 2, 3).reshape(blk, bond, bond)
    local = local_columns(columns, leg_ops, leg_ops.transpose(0, 2, 1), picks, coefs)

    leaving = local.reshape(blk, bond, Y, ZH, C, blk).transpose(3, 2, 4, 0, 5, 1)

    def for_away(shift):
        return lax.dynamic_index_in_dim(leaving, (zh + shift) % ZH, 0, keepdims=False)

    away = jnp.zeros((X, Y, C, blk, blk, bond), BF16)
    for s in (0, 1, 3, 2):
        piece = shifted(for_away(s), s) if s else for_away(s)
        away = lax.dynamic_update_slice_in_dim(away, piece[None], (zh - s) % ZH, 0)

    local_rows = local.reshape(blk, bond // blk, blk, bond).transpose(1, 0, 2, 3)
    said = lax.dynamic_index_in_dim(home_rows, x, 0)[None]
    said = jnp.broadcast_to(said, (X * Y * C, 1, blk, bond))
    both = exchange(jnp.concatenate([home, local_rows, said], axis=1), PLANE)
    bra = both[:, :blk].reshape(bond, blk, bond)
    ket = both[:, blk : 2 * blk].reshape(bond, blk, bond)
    home_p = both[:, 2 * blk].reshape(X, Y, C, blk, bond).transpose(1, 0, 2, 3, 4)
    home_p = home_p.reshape(bond, bond).astype(F32)
    env = jnp.einsum("ulr,vlr->uv", bra, ket, preferred_element_type=F32) / bond
    lifted = jnp.dot(home_p.T, jnp.dot(env, home_p, precision=HIGH), precision=HIGH)
    lifted = exchange(lifted.astype(BF16).reshape(X * Y * C, blk, bond), PLANE)
    lifted = lifted.astype(F32).sum(axis=0).astype(BF16)
    everyone = exchange(jnp.broadcast_to(lifted[None], (ZL * ZH, blk, bond)), LINE)

    far, everyone = tied(legs[2], everyone)
    legs[2] = shifted(far, 2)

    everyone = everyone.astype(F32)
    total = everyone.sum(axis=0)
    mates = lax.dynamic_index_in_dim(
        everyone.reshape(ZL, ZH, blk, bond), zl, 0, keepdims=False
    )
    top_rows = lax.dynamic_slice_in_dim(top_env, plane * blk, blk, 0)
    coupling = ((total + top_rows)[None] - mates).astype(BF16)
    coupling = jnp.broadcast_to(coupling[:, None], (X, Y * C, blk, bond))
    coupling = exchange(coupling.reshape(X * Y * C, blk, bond), PLANE)
    coupling = coupling.reshape(bond, bond).astype(F32)

    split = mates_n * blk
    right = jnp.zeros((Y, C, ZH, blk + 1, blk, bond), BF16)
    for s in (0, 1, 3, 2):
        piece = legs[s][:split].reshape(Y, C, 1, blk, blk, bond)
        row = jnp.broadcast_to(legs[s][split:], (Y, C, 1, 1, blk, bond))
        piece = jnp.concatenate([piece, row], axis=3)
        right = lax.dynamic_update_slice_in_dim(right, piece, (zh - s) % ZH, 2)
    right = exchange(right.reshape(mates_n, ZH, blk + 1, blk, bond), ("y", "c"))
    right = right.reshape(Y, C, ZH, blk + 1, blk, bond).transpose(0, 2, 1, 3, 4, 5)
    lift = right[:, :, :, blk].reshape(bond, bond).astype(F32)
    right = right[:, :, :, :blk].reshape(bond * blk, bond)

    factor = 1.0 / math.sqrt(bond * X * ZL)
    hole = jnp.dot(jnp.dot(lift, coupling, precision=HIGH), lift.T, precision=HIGH)
    hole = (hole * factor).astype(BF16)

    arrived = exchange(away.reshape(X * Y * C, blk, blk, bond), PLANE).reshape(bond, blk, bond)
    arrived = arrived.transpose(2, 1, 0).reshape(bond * blk, bond)
    return result_rows(right, hole, arrived).reshape(1, bond, blk, bond)


def solution(mesh):
    fine = Mesh(mesh.devices.reshape(X, ZL, Y, ZH, C), ("x", "zl", "y", "zh", "c"))
    child, shard = ("x", "zl"), ("y", "zh", "c")
    in_specs = (
        P(child, shard, None, None),
        P(),
        P(child, None, None),
        P(child, None),
        P(child, shard, None),
        P(),
    )
    out_specs = P(child, None, shard, None)
    return jax.shard_map(body, mesh=fine, in_specs=in_specs, out_specs=out_specs, check_vma=False)
```

```python
import math

import jax
import jax.numpy as jnp
from jax import lax
from jax.experimental import pallas as pl
from jax.experimental.pallas import tpu as pltpu
from jax.sharding import Mesh, PartitionSpec as P

X, ZL, Y, ZH, C = 4, 4, 4, 4, 2
SHARD = ("y", "zh", "c")
PLANE = ("x", "y", "c")
HIGH = lax.Precision.HIGHEST
F32 = jnp.float32
BF16 = jnp.bfloat16


def exchange(parts, axes):
    return lax.all_to_all(parts, axes, 0, 0, tiled=True)


def gathered(piece, axis, length):
    at = lax.axis_index(axis)
    whole = jnp.zeros((length, *piece.shape), piece.dtype)
    for shift in range(length):
        moved = piece
        if shift:
            moved = permuted(piece, axis, [(i, (i + shift) % length) for i in range(length)])
        whole = lax.dynamic_update_slice_in_dim(whole, moved[None], (at - shift) % length, 0)
    return whole


def permuted(piece, axis, pairs):
    return lax.ppermute(piece, axis, pairs)


def local_kernel(picks, coefs, tensor, bank, bank_t, out):
    def column(u, carry):
        block = tensor[u]
        total = None
        for term in range(picks.shape[0]):
            left = bank[picks[term, 0]]
            right = bank_t[picks[term, 1]]
            image = jax.lax.dot_general(
                right, block, (((1,), (1,)), ((), ())), preferred_element_type=F32
            ).astype(BF16)
            part = coefs[term] * jnp.dot(image, left, preferred_element_type=F32)
            total = part if total is None else total + part
        out[u] = total.astype(out.dtype)
        return carry

    lax.fori_loop(0, tensor.shape[0], column, 0)


def local_columns(tensor, bank, bank_t, picks, coefs):
    blk, bond, _ = tensor.shape
    flops = 4 * blk * bond**3 * picks.shape[0]
    return pl.pallas_call(
        local_kernel,
        out_shape=jax.ShapeDtypeStruct((blk, bond, bond), BF16),
        in_specs=[pl.BlockSpec(memory_space=pltpu.SMEM)] * 2
        + [pl.BlockSpec(memory_space=pltpu.VMEM)] * 3,
        out_specs=pl.BlockSpec(memory_space=pltpu.VMEM),
        cost_estimate=pl.CostEstimate(
            flops=flops, bytes_accessed=8 * blk * bond * bond, transcendentals=0
        ),
        compiler_params=pltpu.CompilerParams(vmem_limit_bytes=16 * 2**20),
        name="local_columns",
    )(picks, coefs, tensor, bank, bank_t)


def result_kernel(right, hole, arrived, out):
    lines = 256

    def chunk(i, carry):
        at = pl.ds(pl.multiple_of(i * lines, lines), lines)
        moved = jnp.dot(right[at, :], hole[...], preferred_element_type=F32)
        out[at, :] = (arrived[at, :].astype(F32) + moved).astype(out.dtype)
        return carry

    lax.fori_loop(0, right.shape[0] // lines, chunk, 0)


def result_rows(right, hole, arrived):
    rows, bond = right.shape
    return pl.pallas_call(
        result_kernel,
        out_shape=jax.ShapeDtypeStruct((rows, bond), BF16),
        in_specs=[pl.BlockSpec(memory_space=pltpu.VMEM)] * 3,
        out_specs=pl.BlockSpec(memory_space=pltpu.VMEM),
        cost_estimate=pl.CostEstimate(
            flops=2 * rows * bond * bond, bytes_accessed=6 * rows * bond, transcendentals=0
        ),
        compiler_params=pltpu.CompilerParams(vmem_limit_bytes=16 * 2**20),
        name="result_rows",
    )(right, hole, arrived)


def shards(child_tensors, leg_ops, term_ops, term_coef, parent, top_env):
    plane = (lax.axis_index("x") * Y + lax.axis_index("y")) * C + lax.axis_index("c")
    tensor = child_tensors[0]
    blk, bond, _ = tensor.shape
    devices = Y * ZH * C

    turned = tensor.transpose(2, 0, 1).reshape(devices, blk, blk, bond)
    columns = exchange(turned, SHARD).transpose(1, 0, 2, 3).reshape(blk, bond, bond)

    lift = gathered(parent[0], "zh", ZH)

    blocks = tensor.reshape(blk, devices, blk, bond).transpose(1, 0, 2, 3)
    blocks, lift = lax.optimization_barrier((blocks, lift))
    right = exchange(blocks, SHARD).reshape(bond * blk, bond)

    local = local_columns(columns, leg_ops, leg_ops.transpose(0, 2, 1), term_ops[0], term_coef[0])
    local = local.reshape(blk, devices, blk, bond).transpose(1, 0, 2, 3)
    local, right, lift = lax.optimization_barrier((local, right, lift))
    lift = gathered(gathered(lift, "c", C), "y", Y)
    lift = lift.transpose(0, 2, 1, 3, 4).reshape(bond, bond).astype(F32)
    local = exchange(local, SHARD).reshape(bond, blk, bond)
    local = local.transpose(2, 1, 0).reshape(bond * blk, bond)

    env = jnp.einsum("pu,pv->uv", right, local, preferred_element_type=F32) / bond
    lifted = jnp.dot(lift.T, jnp.dot(env, lift, precision=HIGH), precision=HIGH)

    lifted = exchange(lifted.astype(BF16).reshape(X * Y * C, blk, bond), PLANE)
    lifted = lifted.reshape(X, Y * C, blk, bond).astype(F32).sum(axis=1).astype(BF16)
    lifted = exchange(jnp.broadcast_to(lifted[None], (ZH, X, blk, bond)), ("zh",))
    mates = lifted.astype(F32).sum(axis=0)
    total = exchange(jnp.broadcast_to(mates.sum(axis=0)[None], (ZL, blk, bond)), ("zl",))
    total = total.sum(axis=0)
    top_rows = lax.dynamic_slice_in_dim(top_env, plane * blk, blk, 0)
    coupling = ((total + top_rows)[None] - mates).astype(BF16)
    coupling = jnp.broadcast_to(coupling[:, None], (X, Y * C, blk, bond))
    coupling = exchange(coupling.reshape(X * Y * C, blk, bond), PLANE)
    coupling = coupling.reshape(bond, bond).astype(F32)
    factor = 1.0 / math.sqrt(bond * X * ZL)
    hole = jnp.dot(jnp.dot(lift, coupling, precision=HIGH), lift.T, precision=HIGH)
    hole = (hole * factor).astype(BF16)

    return result_rows(right, hole, local).reshape(1, bond, blk, bond)


def solution(mesh):
    fine = Mesh(mesh.devices.reshape(X, ZL, Y, ZH, C), ("x", "zl", "y", "zh", "c"))
    child, shard = ("x", "zl"), ("y", "zh", "c")
    in_specs = (
        P(child, shard, None, None),
        P(),
        P(child, None, None),
        P(child, None),
        P(child, shard, None),
        P(),
    )
    out_specs = P(child, None, shard, None)
    return jax.shard_map(shards, mesh=fine, in_specs=in_specs, out_specs=out_specs, check_vma=False)
```

```python
import math

import jax
import jax.numpy as jnp
from jax import lax
from jax.experimental import pallas as pl
from jax.experimental.pallas import tpu as pltpu
from jax.sharding import Mesh, PartitionSpec as P

X, ZL, Y, ZH, C = 4, 4, 4, 4, 2
SHARD = ("y", "zh", "c")
PLANE = ("x", "y", "c")
LINE = ("zl", "zh")
HIGH = lax.Precision.HIGHEST
F32 = jnp.float32
BF16 = jnp.bfloat16


def exchange(parts, axes):
    return lax.all_to_all(parts, axes, 0, 0, tiled=True)


def gathered(piece, axis, length):
    at = lax.axis_index(axis)
    whole = jnp.zeros((length, *piece.shape), piece.dtype)
    for shift in range(length):
        moved = piece
        if shift:
            moved = permuted(piece, axis, [(i, (i + shift) % length) for i in range(length)])
        whole = lax.dynamic_update_slice_in_dim(whole, moved[None], (at - shift) % length, 0)
    return whole


def permuted(piece, axis, pairs):
    return lax.ppermute(piece, axis, pairs)


def local_kernel(picks, coefs, tensor, bank, bank_t, out):
    def column(u, carry):
        block = tensor[u]
        total = None
        for term in range(picks.shape[0]):
            left = bank[picks[term, 0]]
            right = bank_t[picks[term, 1]]
            image = jax.lax.dot_general(
                right, block, (((1,), (1,)), ((), ())), preferred_element_type=F32
            ).astype(BF16)
            part = coefs[term] * jnp.dot(image, left, preferred_element_type=F32)
            total = part if total is None else total + part
        out[u] = total.astype(out.dtype)
        return carry

    lax.fori_loop(0, tensor.shape[0], column, 0)


def local_columns(tensor, bank, bank_t, picks, coefs):
    blk, bond, _ = tensor.shape
    flops = 4 * blk * bond**3 * picks.shape[0]
    return pl.pallas_call(
        local_kernel,
        out_shape=jax.ShapeDtypeStruct((blk, bond, bond), BF16),
        in_specs=[pl.BlockSpec(memory_space=pltpu.SMEM)] * 2
        + [pl.BlockSpec(memory_space=pltpu.VMEM)] * 3,
        out_specs=pl.BlockSpec(memory_space=pltpu.VMEM),
        cost_estimate=pl.CostEstimate(
            flops=flops, bytes_accessed=8 * blk * bond * bond, transcendentals=0
        ),
        compiler_params=pltpu.CompilerParams(vmem_limit_bytes=16 * 2**20),
        name="local_columns",
    )(picks, coefs, tensor, bank, bank_t)


def result_kernel(right, hole, arrived, out):
    lines = 256

    def chunk(i, carry):
        at = pl.ds(pl.multiple_of(i * lines, lines), lines)
        moved = jnp.dot(right[at, :], hole[...], preferred_element_type=F32)
        out[at, :] = (arrived[at, :].astype(F32) + moved).astype(out.dtype)
        return carry

    lax.fori_loop(0, right.shape[0] // lines, chunk, 0)


def result_rows(right, hole, arrived):
    rows, bond = right.shape
    return pl.pallas_call(
        result_kernel,
        out_shape=jax.ShapeDtypeStruct((rows, bond), BF16),
        in_specs=[pl.BlockSpec(memory_space=pltpu.VMEM)] * 3,
        out_specs=pl.BlockSpec(memory_space=pltpu.VMEM),
        cost_estimate=pl.CostEstimate(
            flops=2 * rows * bond * bond, bytes_accessed=6 * rows * bond, transcendentals=0
        ),
        compiler_params=pltpu.CompilerParams(vmem_limit_bytes=16 * 2**20),
        name="result_rows",
    )(right, hole, arrived)


def shards(child_tensors, leg_ops, term_ops, term_coef, parent, top_env):
    plane = (lax.axis_index("x") * Y + lax.axis_index("y")) * C + lax.axis_index("c")
    tensor = child_tensors[0]
    blk, bond, _ = tensor.shape
    devices = Y * ZH * C

    turned = tensor.transpose(2, 0, 1).reshape(devices, blk, blk, bond)
    columns = exchange(turned, SHARD).transpose(1, 0, 2, 3).reshape(blk, bond, bond)

    lift = gathered(parent[0], "zh", ZH)

    blocks = tensor.reshape(blk, devices, blk, bond).transpose(1, 0, 2, 3)
    blocks, lift = lax.optimization_barrier((blocks, lift))
    right = exchange(blocks, SHARD).reshape(bond * blk, bond)

    local = local_columns(columns, leg_ops, leg_ops.transpose(0, 2, 1), term_ops[0], term_coef[0])
    local = local.reshape(blk, devices, blk, bond).transpose(1, 0, 2, 3)
    local, right, lift = lax.optimization_barrier((local, right, lift))
    lift = gathered(gathered(lift, "c", C), "y", Y)
    lift = lift.transpose(0, 2, 1, 3, 4).reshape(bond, bond).astype(F32)
    local = exchange(local, SHARD).reshape(bond, blk, bond)
    local = local.transpose(2, 1, 0).reshape(bond * blk, bond)

    env = jnp.einsum("pu,pv->uv", right, local, preferred_element_type=F32) / bond
    lifted = jnp.dot(lift.T, jnp.dot(env, lift, precision=HIGH), precision=HIGH)

    lifted = exchange(lifted.astype(BF16).reshape(X * Y * C, blk, bond), PLANE)
    lifted = lifted.reshape(X, Y * C, blk, bond).astype(F32).sum(axis=1).astype(BF16)
    lifted = exchange(jnp.broadcast_to(lifted[None], (ZL * ZH, X, blk, bond)), LINE)
    lifted = lifted.reshape(ZL, ZH, X, blk, bond).astype(F32).sum(axis=1)
    total = lifted.sum(axis=(0, 1))
    mates = lax.dynamic_index_in_dim(lifted, lax.axis_index("zl"), 0, keepdims=False)
    top_rows = lax.dynamic_slice_in_dim(top_env, plane * blk, blk, 0)
    coupling = ((total + top_rows)[None] - mates).astype(BF16)
    coupling = jnp.broadcast_to(coupling[:, None], (X, Y * C, blk, bond))
    coupling = exchange(coupling.reshape(X * Y * C, blk, bond), PLANE)
    coupling = coupling.reshape(bond, bond).astype(F32)
    factor = 1.0 / math.sqrt(bond * X * ZL)
    hole = jnp.dot(jnp.dot(lift, coupling, precision=HIGH), lift.T, precision=HIGH)
    hole = (hole * factor).astype(BF16)

    return result_rows(right, hole, local).reshape(1, bond, blk, bond)


def solution(mesh):
    fine = Mesh(mesh.devices.reshape(X, ZL, Y, ZH, C), ("x", "zl", "y", "zh", "c"))
    child, shard = ("x", "zl"), ("y", "zh", "c")
    in_specs = (
        P(child, shard, None, None),
        P(),
        P(child, None, None),
        P(child, None),
        P(child, shard, None),
        P(),
    )
    out_specs = P(child, None, shard, None)
    return jax.shard_map(shards, mesh=fine, in_specs=in_specs, out_specs=out_specs, check_vma=False)
```

```python
import math

import jax
import jax.numpy as jnp
from jax import lax
from jax.experimental import pallas as pl
from jax.experimental.pallas import tpu as pltpu
from jax.sharding import Mesh, PartitionSpec as P

X, ZL, Y, ZH, C = 4, 4, 4, 4, 2
SHARD = ("y", "zh", "c")
PLANE = ("x", "y", "c")
LINE = ("zl", "zh")
HIGH = lax.Precision.HIGHEST
F32 = jnp.float32
BF16 = jnp.bfloat16


def exchange(parts, axes):
    return lax.all_to_all(parts, axes, 0, 0, tiled=True)


def gathered(piece, axis, length):
    at = lax.axis_index(axis)
    whole = jnp.zeros((length, *piece.shape), piece.dtype)
    for shift in range(length):
        moved = piece
        if shift:
            moved = permuted(piece, axis, [(i, (i + shift) % length) for i in range(length)])
        whole = lax.dynamic_update_slice_in_dim(whole, moved[None], (at - shift) % length, 0)
    return whole


def permuted(piece, axis, pairs):
    return lax.ppermute(piece, axis, pairs)


def local_kernel(picks, coefs, tensor, bank, bank_t, out):
    def column(u, carry):
        block = tensor[u]
        total = None
        for term in range(picks.shape[0]):
            left = bank[picks[term, 0]]
            right = bank_t[picks[term, 1]]
            image = jax.lax.dot_general(
                right, block, (((1,), (1,)), ((), ())), preferred_element_type=F32
            ).astype(BF16)
            part = coefs[term] * jnp.dot(image, left, preferred_element_type=F32)
            total = part if total is None else total + part
        out[u] = total.astype(out.dtype)
        return carry

    lax.fori_loop(0, tensor.shape[0], column, 0)


def local_columns(tensor, bank, bank_t, picks, coefs):
    blk, bond, _ = tensor.shape
    flops = 4 * blk * bond**3 * picks.shape[0]
    return pl.pallas_call(
        local_kernel,
        out_shape=jax.ShapeDtypeStruct((blk, bond, bond), BF16),
        in_specs=[pl.BlockSpec(memory_space=pltpu.SMEM)] * 2
        + [pl.BlockSpec(memory_space=pltpu.VMEM)] * 3,
        out_specs=pl.BlockSpec(memory_space=pltpu.VMEM),
        cost_estimate=pl.CostEstimate(
            flops=flops, bytes_accessed=8 * blk * bond * bond, transcendentals=0
        ),
        compiler_params=pltpu.CompilerParams(vmem_limit_bytes=16 * 2**20),
        name="local_columns",
    )(picks, coefs, tensor, bank, bank_t)


def result_kernel(right, hole, arrived, out):
    lines = 256

    def chunk(i, carry):
        at = pl.ds(pl.multiple_of(i * lines, lines), lines)
        moved = jnp.dot(right[at, :], hole[...], preferred_element_type=F32)
        out[at, :] = (arrived[at, :].astype(F32) + moved).astype(out.dtype)
        return carry

    lax.fori_loop(0, right.shape[0] // lines, chunk, 0)


def result_rows(right, hole, arrived):
    rows, bond = right.shape
    return pl.pallas_call(
        result_kernel,
        out_shape=jax.ShapeDtypeStruct((rows, bond), BF16),
        in_specs=[pl.BlockSpec(memory_space=pltpu.VMEM)] * 3,
        out_specs=pl.BlockSpec(memory_space=pltpu.VMEM),
        cost_estimate=pl.CostEstimate(
            flops=2 * rows * bond * bond, bytes_accessed=6 * rows * bond, transcendentals=0
        ),
        compiler_params=pltpu.CompilerParams(vmem_limit_bytes=16 * 2**20),
        name="result_rows",
    )(right, hole, arrived)


def shards(child_tensors, leg_ops, term_ops, term_coef, parent, top_env):
    plane = (lax.axis_index("x") * Y + lax.axis_index("y")) * C + lax.axis_index("c")
    tensor = child_tensors[0]
    blk, bond, _ = tensor.shape
    devices = Y * ZH * C

    turned = tensor.transpose(2, 0, 1).reshape(devices, blk, blk, bond)
    columns = exchange(turned, SHARD).transpose(1, 0, 2, 3).reshape(blk, bond, bond)

    lift = gathered(parent[0], "zh", ZH)

    blocks = tensor.reshape(blk, devices, blk, bond).transpose(1, 0, 2, 3)

    local = local_columns(columns, leg_ops, leg_ops.transpose(0, 2, 1), term_ops[0], term_coef[0])
    local = local.reshape(blk, devices, blk, bond).transpose(1, 0, 2, 3)
    both, lift = lax.optimization_barrier((jnp.concatenate([blocks, local], axis=1), lift))
    lift = gathered(gathered(lift, "c", C), "y", Y)
    lift = lift.transpose(0, 2, 1, 3, 4).reshape(bond, bond).astype(F32)
    both = exchange(both, SHARD)
    right = both[:, :blk].reshape(bond * blk, bond)
    local = both[:, blk:].reshape(bond, blk, bond)
    local = local.transpose(2, 1, 0).reshape(bond * blk, bond)

    env = jnp.einsum("pu,pv->uv", right, local, preferred_element_type=F32) / bond
    lifted = jnp.dot(lift.T, jnp.dot(env, lift, precision=HIGH), precision=HIGH)

    lifted = exchange(lifted.astype(BF16).reshape(X * Y * C, blk, bond), PLANE)
    lifted = lifted.reshape(X, Y * C, blk, bond).astype(F32).sum(axis=1).astype(BF16)
    lifted = exchange(jnp.broadcast_to(lifted[None], (ZL * ZH, X, blk, bond)), LINE)
    lifted = lifted.reshape(ZL, ZH, X, blk, bond).astype(F32).sum(axis=1)
    total = lifted.sum(axis=(0, 1))
    mates = lax.dynamic_index_in_dim(lifted, lax.axis_index("zl"), 0, keepdims=False)
    top_rows = lax.dynamic_slice_in_dim(top_env, plane * blk, blk, 0)
    coupling = ((total + top_rows)[None] - mates).astype(BF16)
    coupling = jnp.broadcast_to(coupling[:, None], (X, Y * C, blk, bond))
    coupling = exchange(coupling.reshape(X * Y * C, blk, bond), PLANE)
    coupling = coupling.reshape(bond, bond).astype(F32)
    factor = 1.0 / math.sqrt(bond * X * ZL)
    hole = jnp.dot(jnp.dot(lift, coupling, precision=HIGH), lift.T, precision=HIGH)
    hole = (hole * factor).astype(BF16)

    return result_rows(right, hole, local).reshape(1, bond, blk, bond)


def solution(mesh):
    fine = Mesh(mesh.devices.reshape(X, ZL, Y, ZH, C), ("x", "zl", "y", "zh", "c"))
    child, shard = ("x", "zl"), ("y", "zh", "c")
    in_specs = (
        P(child, shard, None, None),
        P(),
        P(child, None, None),
        P(child, None),
        P(child, shard, None),
        P(),
    )
    out_specs = P(child, None, shard, None)
    return jax.shard_map(shards, mesh=fine, in_specs=in_specs, out_specs=out_specs, check_vma=False)
```

```python
import math

import jax
import jax.numpy as jnp
from jax import lax
from jax.experimental import pallas as pl
from jax.experimental.pallas import tpu as pltpu
from jax.sharding import Mesh, PartitionSpec as P

X, ZL, Y, ZH, C = 4, 4, 4, 4, 2
SHARD = ("y", "zh", "c")
PLANE = ("x", "y", "c")
LINE = ("zl", "zh")
HIGH = lax.Precision.HIGHEST
F32 = jnp.float32
BF16 = jnp.bfloat16


def exchange(parts, axes):
    return lax.all_to_all(parts, axes, 0, 0, tiled=True)


def gathered(piece, axis, length):
    at = lax.axis_index(axis)
    whole = jnp.zeros((length, *piece.shape), piece.dtype)
    for shift in range(length):
        moved = piece
        if shift:
            moved = permuted(piece, axis, [(i, (i + shift) % length) for i in range(length)])
        whole = lax.dynamic_update_slice_in_dim(whole, moved[None], (at - shift) % length, 0)
    return whole


def permuted(piece, axis, pairs):
    return lax.ppermute(piece, axis, pairs)


def local_kernel(picks, coefs, tensor, blocks, bank, bank_t, out):
    count, blk, _, bond = tensor.shape

    def column(u, carry):
        block = tensor[:, u].reshape(bond, bond)
        total = None
        for term in range(picks.shape[0]):
            left = bank[picks[term, 0]]
            right = bank_t[picks[term, 1]]
            image = jax.lax.dot_general(
                right, block, (((1,), (1,)), ((), ())), preferred_element_type=F32
            ).astype(BF16)
            part = coefs[term] * jnp.dot(image, left, preferred_element_type=F32)
            total = part if total is None else total + part
        out[:, blk + u] = total.astype(out.dtype).reshape(count, blk, bond)
        out[:, u] = blocks[:, u]
        return carry

    lax.fori_loop(0, blk, column, 0, unroll=2)


def local_columns(tensor, blocks, bank, bank_t, picks, coefs):
    count, blk, _, bond = tensor.shape
    flops = 4 * blk * bond**3 * picks.shape[0]
    return pl.pallas_call(
        local_kernel,
        out_shape=jax.ShapeDtypeStruct((count, 2 * blk, blk, bond), BF16),
        in_specs=[pl.BlockSpec(memory_space=pltpu.SMEM)] * 2
        + [pl.BlockSpec(memory_space=pltpu.VMEM)] * 4,
        out_specs=pl.BlockSpec(memory_space=pltpu.VMEM),
        cost_estimate=pl.CostEstimate(
            flops=flops, bytes_accessed=12 * blk * bond * bond, transcendentals=0
        ),
        compiler_params=pltpu.CompilerParams(vmem_limit_bytes=16 * 2**20),
        name="local_columns",
    )(picks, coefs, tensor, blocks, bank, bank_t)


def result_kernel(right, hole, arrived, out):
    lines = 256

    def chunk(i, carry):
        at = pl.ds(pl.multiple_of(i * lines, lines), lines)
        moved = jnp.dot(right[at, :], hole[...], preferred_element_type=F32)
        out[at, :] = (arrived[at, :].astype(F32) + moved).astype(out.dtype)
        return carry

    lax.fori_loop(0, right.shape[0] // lines, chunk, 0)


def result_rows(right, hole, arrived):
    rows, bond = right.shape
    return pl.pallas_call(
        result_kernel,
        out_shape=jax.ShapeDtypeStruct((rows, bond), BF16),
        in_specs=[pl.BlockSpec(memory_space=pltpu.VMEM)] * 3,
        out_specs=pl.BlockSpec(memory_space=pltpu.VMEM),
        cost_estimate=pl.CostEstimate(
            flops=2 * rows * bond * bond, bytes_accessed=6 * rows * bond, transcendentals=0
        ),
        compiler_params=pltpu.CompilerParams(vmem_limit_bytes=16 * 2**20),
        name="result_rows",
    )(right, hole, arrived)


def shards(child_tensors, leg_ops, term_ops, term_coef, parent, top_env):
    plane = (lax.axis_index("x") * Y + lax.axis_index("y")) * C + lax.axis_index("c")
    tensor = child_tensors[0]
    blk, bond, _ = tensor.shape
    devices = Y * ZH * C

    turned = tensor.transpose(2, 0, 1).reshape(devices, blk, blk, bond)
    columns = exchange(turned, SHARD)

    lift = gathered(parent[0], "zh", ZH)

    blocks = tensor.reshape(blk, devices, blk, bond).transpose(1, 0, 2, 3)

    both = local_columns(
        columns, blocks, leg_ops, leg_ops.transpose(0, 2, 1), term_ops[0], term_coef[0]
    )
    both, lift = lax.optimization_barrier((both, lift))
    lift = gathered(gathered(lift, "c", C), "y", Y)
    lift = lift.transpose(0, 2, 1, 3, 4).reshape(bond, bond).astype(F32)
    both = exchange(both, SHARD)
    right = both[:, :blk].reshape(bond * blk, bond)
    local = both[:, blk:].reshape(bond, blk, bond)
    local = local.transpose(2, 1, 0).reshape(bond * blk, bond)

    env = jnp.einsum("pu,pv->uv", right, local, preferred_element_type=F32) / bond
    lifted = jnp.dot(lift.T, jnp.dot(env, lift, precision=HIGH), precision=HIGH)

    lifted = exchange(lifted.astype(BF16).reshape(X * Y * C, blk, bond), PLANE)
    lifted = lifted.reshape(X, Y * C, blk, bond).astype(F32).sum(axis=1).astype(BF16)
    lifted = exchange(jnp.broadcast_to(lifted[None], (ZL * ZH, X, blk, bond)), LINE)
    lifted = lifted.reshape(ZL, ZH, X, blk, bond).astype(F32).sum(axis=1)
    total = lifted.sum(axis=(0, 1))
    mates = lax.dynamic_index_in_dim(lifted, lax.axis_index("zl"), 0, keepdims=False)
    top_rows = lax.dynamic_slice_in_dim(top_env, plane * blk, blk, 0)
    coupling = ((total + top_rows)[None] - mates).astype(BF16)
    coupling = jnp.broadcast_to(coupling[:, None], (X, Y * C, blk, bond))
    coupling = exchange(coupling.reshape(X * Y * C, blk, bond), PLANE)
    coupling = coupling.reshape(bond, bond).astype(F32)
    factor = 1.0 / math.sqrt(bond * X * ZL)
    hole = jnp.dot(jnp.dot(lift, coupling, precision=HIGH), lift.T, precision=HIGH)
    hole = (hole * factor).astype(BF16)

    return result_rows(right, hole, local).reshape(1, bond, blk, bond)


def solution(mesh):
    fine = Mesh(mesh.devices.reshape(X, ZL, Y, ZH, C), ("x", "zl", "y", "zh", "c"))
    child, shard = ("x", "zl"), ("y", "zh", "c")
    in_specs = (
        P(child, shard, None, None),
        P(),
        P(child, None, None),
        P(child, None),
        P(child, shard, None),
        P(),
    )
    out_specs = P(child, None, shard, None)
    return jax.shard_map(shards, mesh=fine, in_specs=in_specs, out_specs=out_specs, check_vma=False)
```
